256 devices in a mesh: ep: 32 (over z, x), tp: 8 (over y, core).
Axes of the slice: x: 4, y: 4, z: 8, core: 2. Of those that a mesh axis runs over, the one named last changes fastest.
Arguments:
- latents: float32 [8192, 2048], P('ep', 'tp'), may hold values from -6 to 6
- timesteps: int32 [3], replicated, may hold values from 50 to 650, as said below
- routes: int32 [2, 8192, 2], P(None, 'ep'), may hold values from 0 to 31, all different within a row; in each aligned block of 256 rows (0 to 255, 256 to 511, ..., all dimensions but the last counted through in order) at most 24 rows name the same one
- mod_weight: bfloat16 [2048, 3, 2048], P('ep', None, 'tp'), may hold values from -0.125 to 0.125
- router_weight: bfloat16 [2048, 32], replicated, may hold values from -0.125 to 0.125
- up_weight: bfloat16 [32, 2048, 8192], P('ep', None, 'tp'), may hold values from -0.125 to 0.125
- down_weight: bfloat16 [32, 8192, 2048], P('ep', 'tp'), may hold values from -0.0625 to 0.0625
Outputs:
- student_target: float32 [8192, 2048], P('ep', 'tp')
The draws below stay inside these ranges and needn't reach their ends.
Inputs may be any that keep to these rules, and one draw needn't show every extreme that they name: timesteps fall by the same gap of 100 to 150 from each entry to the next; the first lies between 350 and 650. `routes`: the two experts of a token differ; among the 256 tokens of one index of ep in one substep, no expert is named more than 24 times, and in every substep some expert is named exactly 24 times by some index of ep.
All inputs are finite; a program needn't handle non-finite values.
Results may differ from the reference program's by a relative error of at most 0.013.
Values may be sent and summed in bfloat16 or wider, within the bound.
No kernel may reach another device: no remote copies, remote signals or barrier semaphores. Data moves between devices by JAX's collectives and lax.ppermute only.
A program may use at most 64 MiB of HBM per device.

```python
import math
import jax
import jax.numpy as jnp
import numpy as np
from jax import lax

D = 2048
FF = 8192
TOK_DEV = 256
SUBSTEPS = 2
EXPERTS = 32
CAP = 24
TOKENS = 8192
N_EP = 32
N_TP = 8


def draw_timesteps(key, part):
    first_key, second_key = jax.random.split(jax.random.fold_in(key, 11))
    start_value = jax.random.randint(first_key, (), 350, 651)
    gap_value = jax.random.randint(second_key, (), 100, 151)
    return jnp.stack([start_value, start_value - gap_value, start_value - 2 * gap_value]).astype(jnp.int32)


def block_levels(own_key, dims, pieces, low, top_value):
    loudness, own = 1.0, jax.random.fold_in(own_key, 6)
    for position, shards_of in pieces:
        steps = jnp.exp(jax.random.uniform(jax.random.fold_in(own, position), (shards_of,), jnp.float32, low / len(pieces), top_value / len(pieces)))
        loudness = loudness * jnp.repeat(steps, dims[position] // shards_of).reshape([-1 if axis == position else 1 for axis in range(len(dims))])
    return loudness


def routed_block(own_key, own, number, rows, count, top, reach, skew):
    ranking = jax.random.permutation(own_key, count)
    packed, ordinary = portions_of(count, rows * top, reach, skew, True), portions_of(count, rows * top, reach, skew, False)
    places = jnp.arange(count)

    def named(tallies, offset_by):
        used = int((tallies > 0).sum())
        fixed = max(1, used // 4)
        moved = fixed + (places - fixed + offset_by * (used - fixed)) % max(1, count - fixed)
        return jnp.zeros((count,), jnp.int32).at[ranking[jnp.where(places < fixed, places, moved)]].set(jnp.asarray(tallies, jnp.int32))

    tallies = jnp.where(number % 4 == 0, named(packed, number // 4), named(ordinary, number - number // 4 - 1))
    mixed = jax.random.permutation(jax.random.fold_in(own, 3), count)
    source_of, receiver = mixed[0:count // 2 * 2:2], mixed[1:count // 2 * 2:2]
    slack = jnp.minimum(tallies[source_of] - 1, reach - tallies[receiver]) // 2
    slack = jnp.where((source_of == ranking[0]) | (receiver == ranking[0]) | (tallies[receiver] == 0), 0, jnp.maximum(slack, 0))
    moved = jax.random.randint(jax.random.fold_in(own, 4), (count // 2,), 0, 1 << 20) % (slack + 1)
    tallies = tallies.at[source_of].add(-moved).at[receiver].add(moved)
    labels = jnp.searchsorted(jnp.cumsum(tallies), jnp.arange(rows * top), side="right").astype(jnp.int32)
    grid = labels.reshape(top, rows).T
    grid = grid[jax.random.permutation(jax.random.fold_in(own, 1), rows)]
    offset_by = jax.random.randint(jax.random.fold_in(own, 2), (rows, 1), 0, top)
    return jnp.take_along_axis(grid, (jnp.arange(top)[None, :] + offset_by) % top, axis=1)


def portions_of(amount, total, bound, lean, full):
    weights = [(1 << 20) // math.isqrt(rank ** lean) + 1 for rank in range(1, amount + 1)]
    largest = bound if full else min(bound, max(-(-total // amount), total * weights[0] // sum(weights)))
    least = 1 if total - largest >= amount - 1 else 0
    counts, surplus = [largest] + [least] * (amount - 1), total - largest - least * (amount - 1)
    while surplus > 0:
        movable = [i for i in range(1, amount) if counts[i] < largest] or [i for i in range(1, amount) if counts[i] < bound]
        mass, remaining = sum([weights[i] for i in movable]), surplus
        for i in movable:
            extra = min(bound - counts[i], max(1, remaining * weights[i] // mass), surplus)
            counts[i] = counts[i] + extra
            surplus = surplus - extra
    return np.array(counts)


def gaussian(key, extent, scale, bound, shards=(), kind=jnp.bfloat16):
    array = jax.random.normal(key, extent, jnp.float32) * scale
    if len(shards) > 0:
        array = block_levels(key, extent, shards, -0.22, 0.18) * array
    return jnp.clip(array, min=-bound, max=bound).astype(kind)


def setup_inputs(seed: int = 0) -> dict:
    key_of = jax.random.split(jax.random.key(seed), 8)
    latents = gaussian(key_of[0], (TOKENS, D), 1.0, 6.0, ((0, 32), (1, 8)), jnp.float32)
    timesteps = draw_timesteps(jax.random.fold_in(key_of[7], 71), 0)
    routes_keys = jax.random.split(jax.random.fold_in(key_of[2], 1), SUBSTEPS * TOKENS // TOK_DEV)
    routes_turns = jax.random.permutation(jax.random.fold_in(key_of[2], 3), SUBSTEPS * TOKENS // TOK_DEV)
    routes = jax.vmap(lambda own, number: routed_block(jax.random.fold_in(key_of[2], 2), own, number, TOK_DEV, EXPERTS, 2, CAP, 2))(routes_keys, routes_turns).reshape((SUBSTEPS, TOKENS, 2))
    mod_weight = gaussian(key_of[3], (D, 3, D), D ** -0.5, 0.125, ((0, 32), (2, 8)))
    router_weight = gaussian(key_of[4], (D, EXPERTS), D ** -0.5, 0.125)
    up_weight = gaussian(key_of[5], (EXPERTS, D, FF), D ** -0.5, 0.125, ((0, 32), (2, 8)))
    down_weight = gaussian(key_of[6], (EXPERTS, FF, D), FF ** -0.5, 0.0625, ((0, 32), (1, 8)))
    return dict(latents=latents, timesteps=timesteps, routes=routes, mod_weight=mod_weight, router_weight=router_weight, up_weight=up_weight, down_weight=down_weight)


def plan(timestep):
    angle_value = (timestep.astype(jnp.float32) / 1000.0 + 0.008) / 1.008 * (math.pi / 2)
    return (jnp.cos(angle_value), jnp.sin(angle_value))

def embedding(timesteps_pair, width):
    half_width = width // 2
    frequency = jnp.exp(-math.log(10000.0) * jnp.arange(half_width, dtype=jnp.float32) / half_width)
    phases = timesteps_pair.astype(jnp.float32)[:, None] * frequency[None, :]
    return jnp.concatenate([jnp.cos(phases), jnp.sin(phases)], axis=1)

def reference(latents, timesteps, routes, mod_weight, router_weight, up_weight, down_weight):
    condition = embedding(timesteps[:2], D).astype(jnp.bfloat16)
    modulation = jnp.dot(condition, mod_weight.reshape(D, 3 * D), preferred_element_type=jnp.float32).reshape(2, 3, D)
    group_width = FF // N_TP
    most_rows = N_EP * CAP
    expert_ids = jnp.arange(EXPERTS, dtype=jnp.int32)
    current = latents
    for sub_step in range(2):
        cos_now, sin_now = plan(timesteps[sub_step])
        cos_next, sin_next = plan(timesteps[sub_step + 1])
        row_mean = lax.optimization_barrier(jnp.sum(current, axis=1)) / D
        row_var = lax.optimization_barrier(jnp.sum(current * current, axis=1)) / D - row_mean * row_mean
        normed = (current - row_mean[:, None]) * lax.rsqrt(row_var[:, None] + 1e-06)
        shift_row = modulation[sub_step, 0]
        scale_row = modulation[sub_step, 1]
        gate_row = modulation[sub_step, 2]
        full_rows = (normed * (1.0 + scale_row) + shift_row).astype(jnp.bfloat16)
        logits = jnp.dot(full_rows, router_weight, preferred_element_type=jnp.float32)
        chosen = routes[sub_step]
        one_hot = chosen[:, :, None] == expert_ids
        picked = lax.optimization_barrier(jnp.sum(jnp.where(one_hot, logits[:, None, :], jnp.float32(0.0)), axis=2))
        gate_probs = jax.nn.sigmoid(picked)
        weights = gate_probs / lax.optimization_barrier(jnp.sum(gate_probs, axis=1, keepdims=True))
        flat_ids = chosen.reshape(-1)

        def per_expert(pairs, inputs):
            expert_index, up_matrix, down_matrix = inputs
            matches = flat_ids == expert_index
            positions = jnp.nonzero(matches, size=most_rows, fill_value=0)[0].astype(jnp.int32)
            valid = jnp.arange(most_rows, dtype=jnp.int32) < jnp.sum(matches.astype(jnp.int32))
            input_rows = full_rows[positions // 2]
            hidden = jax.nn.gelu(jnp.dot(input_rows, up_matrix, preferred_element_type=jnp.float32)).astype(jnp.bfloat16)
            total = jnp.zeros((most_rows, D), jnp.float32)
            for group in range(N_TP):
                part = jnp.dot(hidden[:, group * group_width:(group + 1) * group_width], down_matrix[group * group_width:(group + 1) * group_width], preferred_element_type=jnp.float32).astype(jnp.bfloat16)
                part = lax.optimization_barrier(part)
                total = total + part.astype(jnp.float32)
            pairs = pairs.at[positions].add(jnp.where(valid[:, None], total, jnp.float32(0.0)))
            return (pairs, None)
        pairs, _ = lax.scan(per_expert, jnp.zeros((2 * TOKENS, D), jnp.float32), (expert_ids, up_weight, down_weight))
        expert_mix = lax.optimization_barrier(jnp.sum(weights[:, :, None] * pairs.reshape(TOKENS, 2, D), axis=1))
        noise_pred = current + gate_row * expert_mix
        clean_estimate = (current - sin_now * noise_pred) / cos_now
        current = cos_next * clean_estimate + sin_next * noise_pred
    cos_first, sin_first = plan(timesteps[0])
    cos_last, sin_last = plan(timesteps[2])
    sigma_ratio = sin_last / sin_first
    return (current - sigma_ratio * latents) / (cos_last - sigma_ratio * cos_first)
```

```python
import math

import jax
import jax.numpy as jnp
from jax import lax
from jax.sharding import PartitionSpec as P


CORES = 2
HALVES = 2


def plan(timestep):
    angle_value = (timestep.astype(jnp.float32) / 1000.0 + 0.008) / 1.008 * (math.pi / 2)
    return (jnp.cos(angle_value), jnp.sin(angle_value))


def embedding(timesteps_pair, width):
    half_width = width // 2
    frequency = jnp.exp(-math.log(10000.0) * jnp.arange(half_width, dtype=jnp.float32) / half_width)
    phases = timesteps_pair.astype(jnp.float32)[:, None] * frequency[None, :]
    return jnp.concatenate([jnp.cos(phases), jnp.sin(phases)], axis=1)


def shifted(array, rows_away, other_core):
    n_tp = lax.axis_size("tp")
    n_y = n_tp // CORES
    pairs = []
    for i in range(n_tp):
        y, core = divmod(i, CORES)
        pairs.append((i, ((y + rows_away) % n_y) * CORES + (core ^ other_core)))
    return lax.ppermute(array, "tp", pairs)


def summed_by_permutes(array):
    n_y = lax.axis_size("tp") // CORES
    total = array
    for core in range(CORES):
        for away in range(n_y):
            if core or away:
                total = total + shifted(array, away, core)
    return total


def summed_at_once(array, axis):
    length = lax.axis_size(axis)
    everything = lax.all_to_all(
        jnp.broadcast_to(array[None], (length, *array.shape)), axis, 0, 0, tiled=True
    )
    return everything.sum(axis=0)


def expert_rows(rows, up_rel, down_rel):
    n_y = lax.axis_size("tp") // CORES
    width = rows.shape[1]
    own = [rows] + [shifted(rows, -away, 0) for away in range(1, n_y)]
    partner = [shifted(block, 0, 1) for block in own]
    whole = jnp.concatenate(own + partner, axis=1)
    hidden = jax.nn.gelu(jnp.dot(whole, up_rel, preferred_element_type=jnp.float32)).astype(
        jnp.bfloat16
    )
    split = n_y * width
    for_partner = jnp.dot(hidden, down_rel[:, :split], preferred_element_type=jnp.float32).astype(
        jnp.bfloat16
    )
    from_partner = shifted(for_partner, 0, 1)
    mine = jnp.dot(hidden, down_rel[:, split:], preferred_element_type=jnp.float32).astype(
        jnp.bfloat16
    )
    both = mine.astype(jnp.float32) + from_partner.astype(jnp.float32)
    total = both[:, :width]
    for away in range(1, n_y):
        block = both[:, away * width : (away + 1) * width].astype(jnp.bfloat16)
        total = total + shifted(block, away, 0).astype(jnp.float32)
    return total.astype(jnp.bfloat16)


def per_device(latents, timesteps, routes, mod_weight, router_weight, up_weight, down_weight):
    tok_rows, slice_width = latents.shape
    model_width = router_weight.shape[0]
    experts_all = router_weight.shape[1]
    capacity = 3 * tok_rows // experts_all
    slots = experts_all * capacity
    mod_rows = mod_weight.shape[0]
    n_tp = lax.axis_size("tp")
    n_y = n_tp // CORES
    tp_index = lax.axis_index("tp")
    my_y, my_core = tp_index // CORES, tp_index % CORES

    condition = embedding(timesteps[:2], model_width).astype(jnp.bfloat16)
    cond_rows = lax.dynamic_slice_in_dim(condition, lax.axis_index("ep") * mod_rows, mod_rows, 1)
    mod_part = jnp.einsum("sd,dkf->skf", cond_rows, mod_weight, preferred_element_type=jnp.float32)
    first = summed_at_once(mod_part[0, :2], "ep")
    rest = summed_at_once(jnp.concatenate([mod_part[0, 2:], mod_part[1]]), "ep")
    modulation = ((first[0], first[1], rest[0]), (rest[1], rest[2], rest[3]))

    router_rows = lax.dynamic_slice_in_dim(router_weight, tp_index * slice_width, slice_width, 0)

    def feature_block(away, other_core):
        return ((my_y + away) % n_y) * CORES + (my_core ^ other_core)

    up = up_weight[0]
    down = down_weight[0]
    up_rel = jnp.concatenate(
        [
            lax.dynamic_slice_in_dim(up, feature_block(a, o) * slice_width, slice_width, 0)
            for o in range(CORES)
            for a in range(n_y)
        ],
        axis=0,
    )
    down_rel = jnp.concatenate(
        [
            lax.dynamic_slice_in_dim(down, feature_block(a, 1 - o) * slice_width, slice_width, 1)
            for o in range(CORES)
            for a in range(n_y)
        ],
        axis=1,
    )

    expert_ids = jnp.arange(experts_all, dtype=jnp.int32)
    pairs_all = 2 * tok_rows
    earlier = (
        jnp.arange(pairs_all)[:, None] > jnp.arange(pairs_all)[None, :]
    ).astype(jnp.bfloat16)
    flat_hot = routes.reshape(2, pairs_all)[:, :, None] == expert_ids
    both_hot = jnp.concatenate([flat_hot[0], flat_hot[1]], axis=1).astype(jnp.bfloat16)
    before = jnp.dot(earlier, both_hot, preferred_element_type=jnp.float32)
    places = []
    for sub_step in range(2):
        hot = flat_hot[sub_step].astype(jnp.float32)
        own_before = before[:, sub_step * experts_all : (sub_step + 1) * experts_all]
        slot = jnp.sum(own_before * hot, axis=1).astype(jnp.int32)
        places.append((routes[sub_step].reshape(-1) * capacity + slot).reshape(tok_rows, 2))
    slot_ids = jnp.arange(slots, dtype=jnp.int32)

    current = latents
    for sub_step in range(2):
        cos_now, sin_now = plan(timesteps[sub_step])
        cos_next, sin_next = plan(timesteps[sub_step + 1])
        sums = jnp.stack([jnp.sum(current, axis=1), jnp.sum(current * current, axis=1)])
        sums = summed_by_permutes(sums) if sub_step == 0 else summed_at_once(sums, "tp")
        row_mean = sums[0] / model_width
        row_var = sums[1] / model_width - row_mean * row_mean
        normed = (current - row_mean[:, None]) * lax.rsqrt(row_var[:, None] + 1e-06)
        shift_row, scale_row, gate_row = modulation[sub_step]
        modulated = (normed * (1.0 + scale_row) + shift_row).astype(jnp.bfloat16)
        place = places[sub_step]
        goes = (place[:, 0][None, :] == slot_ids[:, None]) | (
            place[:, 1][None, :] == slot_ids[:, None]
        )
        outgoing = jnp.dot(
            goes.astype(jnp.bfloat16), modulated, preferred_element_type=jnp.float32
        ).astype(jnp.bfloat16)
        arrived = lax.all_to_all(
            outgoing.reshape(experts_all, capacity, slice_width), "ep", 0, 0, tiled=True
        ).reshape(slots, slice_width)
        half = slots // HALVES
        done = [
            expert_rows(arrived[h * half : (h + 1) * half], up_rel, down_rel)
            for h in range(HALVES)
        ]
        part_logits = jnp.dot(modulated, router_rows, preferred_element_type=jnp.float32)
        one_hot = routes[sub_step][:, :, None] == expert_ids
        picked = jnp.sum(jnp.where(one_hot, part_logits[:, None, :], 0.0), axis=2)
        picked = summed_at_once(picked.T, "tp").T
        gate_probs = jax.nn.sigmoid(picked)
        weights = gate_probs / jnp.sum(gate_probs, axis=1, keepdims=True)
        returned = lax.all_to_all(
            jnp.concatenate(done).reshape(experts_all, capacity, slice_width),
            "ep",
            0,
            0,
            tiled=True,
        ).reshape(slots, slice_width)
        expert_mix = 0.0
        for k in range(2):
            comes = (place[:, k][:, None] == slot_ids[None, :]).astype(jnp.bfloat16)
            row = jnp.dot(comes, returned, preferred_element_type=jnp.float32)
            expert_mix = expert_mix + weights[:, k][:, None] * row
        noise_pred = current + gate_row * expert_mix
        clean_estimate = (current - sin_now * noise_pred) / cos_now
        current = cos_next * clean_estimate + sin_next * noise_pred
    cos_first, sin_first = plan(timesteps[0])
    cos_last, sin_last = plan(timesteps[2])
    sigma_ratio = sin_last / sin_first
    return (current - sigma_ratio * latents) / (cos_last - sigma_ratio * cos_first)


def solution(mesh):
    in_specs = (
        P("ep", "tp"),
        P(),
        P(None, "ep", None),
        P("ep", None, "tp"),
        P(),
        P("ep", None, "tp"),
        P("ep", "tp", None),
    )
    out_specs = P("ep", "tp")
    return jax.shard_map(
        per_device, mesh=mesh, in_specs=in_specs, out_specs=out_specs, check_vma=False
    )
```

```python
import math

import jax
import jax.numpy as jnp
from jax import lax
from jax.experimental import pallas as pl
from jax.experimental.pallas import tpu as pltpu
from jax.sharding import PartitionSpec as P

CORES = 2
N_Y = 4
CHUNK = 256
LIMIT = 32 * 1024 * 1024


def plan(timestep):
    angle_value = (timestep.astype(jnp.float32) / 1000.0 + 0.008) / 1.008 * (math.pi / 2)
    return (jnp.cos(angle_value), jnp.sin(angle_value))


def embedding(timesteps_pair, width):
    half_width = width // 2
    frequency = jnp.exp(-math.log(10000.0) * jnp.arange(half_width, dtype=jnp.float32) / half_width)
    phases = timesteps_pair.astype(jnp.float32)[:, None] * frequency[None, :]
    return jnp.concatenate([jnp.cos(phases), jnp.sin(phases)], axis=1)


def sent(array, away, other_core=0):
    n_tp = lax.axis_size("tp")
    n_y = n_tp // CORES
    pairs = []
    for i in range(n_tp):
        y, core = divmod(i, CORES)
        pairs.append((i, ((y + away) % n_y) * CORES + (core ^ other_core)))
    return lax.ppermute(array, "tp", pairs)


def swapped(array):
    return sent(array, 0, 1)


def summed_by_permutes(array):
    array = array + swapped(array)
    return array + sent(array, 2) + sent(array, 1) + sent(array, -1)


def summed_at_once(array, axis):
    length = lax.axis_size(axis)
    everything = lax.all_to_all(
        jnp.broadcast_to(array[None], (length, *array.shape)), axis, 0, 0, tiled=True
    )
    return everything.sum(axis=0)


def place(here, away, core, width):
    start = (((here + away) % N_Y) * CORES + core) * width
    return pl.ds(pl.multiple_of(start, width), width)


def dot(a, b):
    return jnp.dot(a, b, preferred_element_type=jnp.float32)


def near_up_kernel(at_ref, own, left, right, own_p, left_p, right_p, up_ref, out_ref):
    here, core = at_ref[0], at_ref[1]
    width = own.shape[1]
    parts = ((own, 0, core), (own_p, 0, 1 - core), (left, -1, core), (left_p, -1, 1 - core))
    parts += ((right, 1, core), (right_p, 1, 1 - core))
    for start in range(0, out_ref.shape[1], CHUNK):
        total = None
        for rows, away, of_core in parts:
            term = dot(
                rows[...], up_ref[place(here, away, of_core, width), start : start + CHUNK]
            )
            total = term if total is None else total + term
        out_ref[:, start : start + CHUNK] = total


def far_kernel(at_ref, near, far_a, far_b, far_pa, far_pb, up_ref, down_ref, hidden, mine, other):
    here, core = at_ref[0], at_ref[1]
    half, width = far_a.shape
    for start in range(0, hidden.shape[1], CHUNK):
        cols = slice(start, start + CHUNK)
        weights = up_ref[place(here, 2, core, width), cols]
        weights_p = up_ref[place(here, 2, 1 - core, width), cols]
        for first, rows, rows_p in ((0, far_a, far_pa), (half, far_b, far_pb)):
            total = near[first : first + half, cols] + (
                dot(rows[...], weights) + dot(rows_p[...], weights_p)
            )
            hidden[first : first + half, cols] = jax.nn.gelu(total).astype(jnp.bfloat16)
    other[...] = dot(hidden[...], down_ref[:, place(here, 2, 1 - core, width)]).astype(jnp.bfloat16)
    mine[...] = dot(hidden[...], down_ref[:, place(here, 2, core, width)]).astype(jnp.bfloat16)


def plus(a, b):
    return a.astype(jnp.float32) + b.astype(jnp.float32)


def add_halves_kernel(a_ref, b_ref, top_ref, bottom_ref):
    half = top_ref.shape[0]
    total = plus(a_ref[...], b_ref[...]).astype(jnp.bfloat16)
    top_ref[...] = total[:half]
    bottom_ref[...] = total[half:]


def near_partner_kernel(at_ref, hidden, down_ref, out_ref):
    here, core = at_ref[0], at_ref[1]
    for k, away in enumerate((1, -1, 0)):
        out_ref[k] = dot(
            hidden[...], down_ref[:, place(here, away, 1 - core, out_ref.shape[2])]
        ).astype(jnp.bfloat16)


def near_own_kernel(at_ref, hidden, down_ref, partner, right, left, own):
    here, core = at_ref[0], at_ref[1]
    for k, (away, out_ref) in enumerate(((1, right), (-1, left), (0, own))):
        product = dot(hidden[...], down_ref[:, place(here, away, core, own.shape[1])])
        out_ref[...] = plus(product.astype(jnp.bfloat16), partner[k]).astype(jnp.bfloat16)


def relay_kernel(right, left, passing_up, passing_down, right_out, left_out):
    half = passing_up.shape[0]
    right_out[:half] = plus(right[:half], passing_up[...]).astype(jnp.bfloat16)
    right_out[half:] = right[half:]
    left_out[:half] = left[:half]
    left_out[half:] = plus(left[half:], passing_down[...]).astype(jnp.bfloat16)


def sum_kernel(own, a, b, out_ref):
    out_ref[...] = (plus(own[...], a[...]) + b[...].astype(jnp.float32)).astype(jnp.bfloat16)


VMEM = pl.BlockSpec(memory_space=pltpu.VMEM)
SMEM = pl.BlockSpec(memory_space=pltpu.SMEM)


def call(kernel, shapes, *operands, blocks=0, transcendentals=0):
    slots, width, hidden = 768, 256, 1024
    return pl.pallas_call(
        kernel,
        in_specs=[SMEM if o.dtype == jnp.int32 else VMEM for o in operands],
        out_specs=[VMEM] * len(shapes),
        out_shape=[jax.ShapeDtypeStruct(s, d) for s, d in shapes],
        compiler_params=pltpu.CompilerParams(vmem_limit_bytes=LIMIT),
        cost_estimate=pl.CostEstimate(
            flops=max(2 * blocks * slots * width * hidden, slots * width),
            bytes_accessed=0,
            transcendentals=transcendentals,
        ),
    )(*operands)


def expert_block(arrived, up, down, at):
    slots, width = arrived.shape
    hidden_width = up.shape[1]
    half = slots // 2
    bf16 = jnp.bfloat16
    block, half_block = ((slots, width), bf16), ((half, width), bf16)
    left, right = sent(arrived, 1), sent(arrived, -1)
    own_p = swapped(arrived)
    far_a, far_b = sent(left[:half], 1), sent(right[half:], -1)
    left_p, right_p = swapped(left), swapped(right)
    (near,) = call(
        near_up_kernel,
        [((slots, hidden_width), jnp.float32)],
        at, arrived, left, right, own_p, left_p, right_p, up,
        blocks=6,
    )
    hidden, mine, other = call(
        far_kernel,
        [((slots, hidden_width), bf16), block, block],
        at, near, far_a, far_b, swapped(far_a), swapped(far_b), up, down,
        blocks=4, transcendentals=slots * hidden_width,
    )
    top, bottom = call(add_halves_kernel, [half_block, half_block], mine, swapped(other))
    passing_up, passing_down = sent(top, 1), sent(bottom, -1)
    (partner,) = call(
        near_partner_kernel, [((3, slots, width), bf16)], at, hidden, down, blocks=3
    )
    to_right, to_left, own = call(
        near_own_kernel, [block] * 3, at, hidden, down, swapped(partner), blocks=3
    )
    to_right, to_left = call(
        relay_kernel, [block, block], to_right, to_left, passing_up, passing_down
    )
    (total,) = call(sum_kernel, [block], own, sent(to_right, 1), sent(to_left, -1))
    return total, own_p


def after(array, *others):
    return lax.optimization_barrier((array, *others))[0]


def per_device(latents, timesteps, routes, mod_weight, router_weight, up_weight, down_weight):
    tok_rows, slice_width = latents.shape
    model_width = router_weight.shape[0]
    experts_all = router_weight.shape[1]
    capacity = 3 * tok_rows // experts_all
    slots = experts_all * capacity
    mod_rows = mod_weight.shape[0]
    tp_index = lax.axis_index("tp")

    condition = embedding(timesteps[:2], model_width).astype(jnp.bfloat16)
    cond_rows = lax.dynamic_slice_in_dim(condition, lax.axis_index("ep") * mod_rows, mod_rows, 1)
    mod_part = jnp.einsum("sd,dkf->skf", cond_rows, mod_weight, preferred_element_type=jnp.float32)
    modulation = summed_at_once(mod_part, "ep")

    router_rows = lax.dynamic_slice_in_dim(router_weight, tp_index * slice_width, slice_width, 0)

    at = jnp.stack([tp_index // CORES, tp_index % CORES])

    expert_ids = jnp.arange(experts_all, dtype=jnp.int32)
    pairs_all = 2 * tok_rows
    earlier = (
        jnp.arange(pairs_all)[:, None] > jnp.arange(pairs_all)[None, :]
    ).astype(jnp.bfloat16)
    flat_hot = routes.reshape(2, pairs_all)[:, :, None] == expert_ids
    both_hot = jnp.concatenate([flat_hot[0], flat_hot[1]], axis=1).astype(jnp.bfloat16)
    before = jnp.dot(earlier, both_hot, preferred_element_type=jnp.float32)
    places = []
    for sub_step in range(2):
        hot = flat_hot[sub_step].astype(jnp.float32)
        own_before = before[:, sub_step * experts_all : (sub_step + 1) * experts_all]
        slot = jnp.sum(own_before * hot, axis=1).astype(jnp.int32)
        places.append((routes[sub_step].reshape(-1) * capacity + slot).reshape(tok_rows, 2))
    slot_ids = jnp.arange(slots, dtype=jnp.int32)

    current = latents
    for sub_step in range(2):
        cos_now, sin_now = plan(timesteps[sub_step])
        cos_next, sin_next = plan(timesteps[sub_step + 1])
        shift_row, scale_row, gate_row = (modulation[sub_step, c] for c in range(3))
        sums = jnp.stack([jnp.sum(current, axis=1), jnp.sum(current * current, axis=1)])
        sums = summed_by_permutes(sums) if sub_step == 0 else summed_at_once(sums, "tp")
        row_mean = sums[0] / model_width
        row_var = sums[1] / model_width - row_mean * row_mean
        normed = (current - row_mean[:, None]) * lax.rsqrt(row_var[:, None] + 1e-06)
        modulated = (normed * (1.0 + scale_row) + shift_row).astype(jnp.bfloat16)
        spot = places[sub_step]
        goes = (spot[:, 0][None, :] == slot_ids[:, None]) | (
            spot[:, 1][None, :] == slot_ids[:, None]
        )
        outgoing = jnp.dot(
            goes.astype(jnp.bfloat16), modulated, preferred_element_type=jnp.float32
        ).astype(jnp.bfloat16)
        arrived = lax.all_to_all(
            outgoing.reshape(experts_all, capacity, slice_width), "ep", 0, 0, tiled=True
        ).reshape(slots, slice_width)
        done, begun = expert_block(arrived, up_weight[0], down_weight[0], at)
        part_logits = jnp.dot(modulated, router_rows, preferred_element_type=jnp.float32)
        one_hot = routes[sub_step][:, :, None] == expert_ids
        picked = jnp.sum(jnp.where(one_hot, part_logits[:, None, :], 0.0), axis=2)
        picked = summed_by_permutes(after(picked.T, begun)).T
        gate_probs = jax.nn.sigmoid(picked)
        weights = gate_probs / jnp.sum(gate_probs, axis=1, keepdims=True)
        returned = lax.all_to_all(
            done.reshape(experts_all, capacity, slice_width),
            "ep",
            0,
            0,
            tiled=True,
        ).reshape(slots, slice_width)
        expert_mix = 0.0
        for k in range(2):
            comes = (spot[:, k][:, None] == slot_ids[None, :]).astype(jnp.bfloat16)
            row = jnp.dot(comes, returned, preferred_element_type=jnp.float32)
            expert_mix = expert_mix + weights[:, k][:, None] * row
        noise_pred = current + gate_row * expert_mix
        clean_estimate = (current - sin_now * noise_pred) / cos_now
        current = cos_next * clean_estimate + sin_next * noise_pred
    cos_first, sin_first = plan(timesteps[0])
    cos_last, sin_last = plan(timesteps[2])
    sigma_ratio = sin_last / sin_first
    return (current - sigma_ratio * latents) / (cos_last - sigma_ratio * cos_first)


def solution(mesh):
    in_specs = (
        P("ep", "tp"),
        P(),
        P(None, "ep", None),
        P("ep", None, "tp"),
        P(),
        P("ep", None, "tp"),
        P("ep", "tp", None),
    )
    out_specs = P("ep", "tp")
    return jax.shard_map(
        per_device, mesh=mesh, in_specs=in_specs, out_specs=out_specs, check_vma=False
    )
```
